32 devices in a mesh: dp: 1 (over z), ing: 4 (over y), grp: 8 (over x, core).
Axes of the slice: x: 4, y: 4, z: 1, core: 2. Of those that a mesh axis runs over, the one named last changes fastest.
The devices are a block of a 4x4x8 slice.
Arguments:
- tokens: bfloat16 [32768, 2048], P(('dp', 'grp', 'ing'))
- expert_ids: int32 [32768, 8], P(('dp', 'grp', 'ing'))
- gate_weights: float32 [32768, 8], P(('dp', 'grp', 'ing'))
- w_gate: bfloat16 [64, 2048, 1024], P(('grp', 'ing'))
- w_up: bfloat16 [64, 2048, 1024], P(('grp', 'ing'))
- w_down: bfloat16 [64, 1024, 2048], P(('grp', 'ing'))
Outputs:
- output: bfloat16 [32768, 2048], P(('dp', 'grp', 'ing'))
All inputs are finite; a program needn't handle non-finite values.
Results may differ from the reference program's by a relative error of at most 0.00163.
Values are sent between devices in bfloat16 or wider.
A program may use at most 768 MiB of HBM per device.

```python
import jax
import jax.numpy as jnp
from jax import lax

TOKENS = 1024
MODEL_DIM = 2048
EXPERT_FF = 1024
EXPERTS = 64
TOP_K = 8
GROUPS = 8
INNER = 4

GROUP_LIMIT = min(GROUPS // 2, TOP_K // 2)
PER_GROUP = TOP_K // GROUP_LIMIT
GROUP_EXPERTS = EXPERTS // GROUPS
GROUP_CAP = 3 * TOKENS * GROUP_LIMIT // (2 * GROUPS)
EXPERT_CAP = (GROUP_CAP * PER_GROUP + GROUP_EXPERTS - 1) // GROUP_EXPERTS
SOURCES = GROUPS * INNER


def draw_routing(route_key, hot_group):
    key_order, key_cycle, key_perm = jax.random.split(route_key, 3)
    token_order = jax.random.permutation(key_order, TOKENS)
    cycle_shift = jax.random.randint(key_cycle, (), 0, GROUPS - 1)
    expert_perm = jax.random.permutation(key_perm, GROUP_EXPERTS)
    rank_ids = jnp.arange(TOKENS)
    hot_token = rank_ids < GROUP_CAP
    slot_ids = jnp.arange(GROUP_LIMIT)[None, :]
    copy_start = rank_ids * GROUP_LIMIT - jnp.minimum(rank_ids, GROUP_CAP)
    copy_index = copy_start[:, None] + slot_ids - hot_token[:, None].astype(jnp.int32)
    other_group = (hot_group + 1 + (copy_index + cycle_shift) % (GROUPS - 1)) % GROUPS
    chosen = jnp.where(hot_token[:, None] & (slot_ids == 0), hot_group, other_group)
    member = jnp.any(chosen[:, :, None] == jnp.arange(GROUPS), axis=1).astype(jnp.int32)
    before = jnp.cumsum(member, axis=0) - member
    earlier = jnp.take_along_axis(before, chosen, axis=1)
    local_slot = (earlier[:, :, None] * PER_GROUP + jnp.arange(PER_GROUP)) % GROUP_EXPERTS
    expert_ids = chosen[:, :, None] * GROUP_EXPERTS + expert_perm[local_slot]
    return expert_ids.reshape(TOKENS, TOP_K)[token_order].astype(jnp.int32)


def setup_inputs(seed: int = 0, part: int = 0) -> dict:
    part_key = jax.random.fold_in(jax.random.key(seed), part)
    key_tokens, key_route, key_hot, key_gate = jax.random.split(part_key, 4)
    key_wg, key_wu, key_wd = jax.random.split(jax.random.key(seed + 1), 3)
    num_rows = SOURCES * TOKENS
    hot_group = jax.random.randint(key_hot, (), 0, GROUPS)
    route_keys = jax.random.split(key_route, SOURCES)
    expert_ids = jax.vmap(draw_routing, in_axes=(0, None))(route_keys, hot_group)
    expert_ids = expert_ids.reshape(num_rows, TOP_K)
    tokens = jax.random.normal(key_tokens, (num_rows, MODEL_DIM), jnp.float32).astype(jnp.bfloat16)
    gate_logits = 0.5 * jax.random.normal(key_gate, (num_rows, TOP_K), jnp.float32)
    gate_weights = jax.nn.softmax(gate_logits, axis=-1)
    w_gate = (jax.random.normal(key_wg, (EXPERTS, MODEL_DIM, EXPERT_FF), jnp.float32) * MODEL_DIM ** -0.5).astype(jnp.bfloat16)
    w_up = (jax.random.normal(key_wu, (EXPERTS, MODEL_DIM, EXPERT_FF), jnp.float32) * MODEL_DIM ** -0.5).astype(jnp.bfloat16)
    w_down = (jax.random.normal(key_wd, (EXPERTS, EXPERT_FF, MODEL_DIM), jnp.float32) * (2.0 * EXPERT_FF ** -0.5)).astype(jnp.bfloat16)
    return {'tokens': tokens, 'expert_ids': expert_ids, 'gate_weights': gate_weights, 'w_gate': w_gate, 'w_up': w_up, 'w_down': w_down}


def expert_block(expert_rows, gate_w, up_w, down_w):
    act_gate = jnp.dot(expert_rows, gate_w, preferred_element_type=jnp.float32)
    act_up = jnp.dot(expert_rows, up_w, preferred_element_type=jnp.float32)
    hidden = (jax.nn.silu(act_gate) * act_up).astype(jnp.bfloat16)
    return jnp.dot(hidden, down_w, preferred_element_type=jnp.float32).astype(jnp.bfloat16)


def reference(tokens, expert_ids, gate_weights, w_gate, w_up, w_down):
    num_rows = tokens.shape[0]
    row_cap = SOURCES * EXPERT_CAP
    row_index = jnp.arange(num_rows, dtype=jnp.int32)

    def one_expert(expert):
        hit_mask = expert_ids == expert
        picked = jnp.any(hit_mask, axis=1)
        gate_row = jnp.sum(jnp.where(hit_mask, gate_weights, 0.0), axis=1)
        picked_int = picked.astype(jnp.int32)
        slot_pos = jnp.where(picked, jnp.cumsum(picked_int) - 1, row_cap)
        row_ids = jnp.full((row_cap,), num_rows, jnp.int32).at[slot_pos].set(row_index, mode='drop')
        expert_rows = jnp.take(tokens, row_ids, axis=0, mode='fill', fill_value=0)
        expert_out = expert_block(expert_rows, w_gate[expert], w_up[expert], w_down[expert])
        row_gate = jnp.take(gate_row, row_ids, axis=0, mode='fill', fill_value=0)
        return row_ids, expert_out.astype(jnp.float32) * row_gate[:, None]

    def group_step(running, group_id):
        def expert_step(group_acc, local_id):
            row_ids, scaled = one_expert(group_id * GROUP_EXPERTS + local_id)
            return group_acc.at[row_ids].add(scaled, mode='drop'), None
        group_acc = lax.scan(expert_step, jnp.zeros((num_rows, MODEL_DIM), jnp.float32), jnp.arange(GROUP_EXPERTS))[0]
        return running + group_acc.astype(jnp.bfloat16).astype(jnp.float32), None

    running = lax.scan(group_step, jnp.zeros((num_rows, MODEL_DIM), jnp.float32), jnp.arange(GROUPS))[0]
    return running.astype(jnp.bfloat16)
```

```python
import functools

import jax
import jax.numpy as jnp
from jax import lax
from jax.experimental import pallas as pl
from jax.experimental.pallas import tpu as pltpu
from jax.sharding import PartitionSpec as P


LANES = 128


def cap_sizes(tokens_dev, top_k, groups, group_exp):
    group_limit = min(groups // 2, top_k // 2)
    per_group = top_k // group_limit
    group_cap = 3 * tokens_dev * group_limit // (2 * groups)
    expert_cap = (group_cap * per_group + group_exp - 1) // group_exp
    return per_group, expert_cap


def ffn_kernel(x_ref, gate_ref, up_ref, down_a_ref, down_b_ref, out_ref):
    rows = x_ref[...]
    act_gate = jnp.dot(rows, gate_ref[...], preferred_element_type=jnp.float32)
    act_up = jnp.dot(rows, up_ref[...], preferred_element_type=jnp.float32)
    hidden = (act_gate * jax.nn.sigmoid(act_gate) * act_up).astype(jnp.bfloat16)
    half = down_a_ref.shape[1]
    for part, down_ref in enumerate((down_a_ref, down_b_ref)):
        out = jnp.dot(hidden, down_ref[...], preferred_element_type=jnp.float32)
        out = out.astype(jnp.bfloat16).reshape(out.shape[0], half // LANES, LANES)
        out_ref[:, part * (half // LANES):(part + 1) * (half // LANES), :] = out


def expert_ffn(rows, gate_w, up_w, down_a, down_b, tile):
    count, dim = rows.shape
    ff = gate_w.shape[1]
    half = down_a.shape[1]
    fixed = lambda i: (0, 0)
    return pl.pallas_call(
        ffn_kernel,
        grid=(count // tile,),
        in_specs=[
            pl.BlockSpec((tile, dim), lambda i: (i, 0)),
            pl.BlockSpec((dim, ff), fixed),
            pl.BlockSpec((dim, ff), fixed),
            pl.BlockSpec((ff, half), fixed),
            pl.BlockSpec((ff, half), fixed),
        ],
        out_specs=pl.BlockSpec((tile, dim // LANES, LANES), lambda i: (i, 0, 0)),
        out_shape=jax.ShapeDtypeStruct((count, dim // LANES, LANES), jnp.bfloat16),
        compiler_params=pltpu.CompilerParams(vmem_limit_bytes=56 * 2**20),
        cost_estimate=pl.CostEstimate(flops=6 * count * dim * ff, bytes_accessed=4 * count * dim + 6 * dim * ff, transcendentals=count * ff),
    )(rows, gate_w, up_w, down_a, down_b)


def combine_kernel(per_group, top_k, pos_ref, gate_ref, *refs):
    sources, (out_ref, held, sems) = refs[:-3], refs[-3:]
    count = sources[0].shape[0]
    copies = [pltpu.make_async_copy(src, held.at[pl.ds(k * count, count)], sems.at[k]) for k, src in enumerate(sources)]
    for copy in copies:
        copy.start()
    for copy in copies:
        copy.wait()

    def one_token(tok, carry):
        total = None
        for first in range(0, top_k, per_group):
            partial = None
            for j in range(first, first + per_group):
                scaled = held[pos_ref[tok * top_k + j]].astype(jnp.float32) * gate_ref[tok * top_k + j]
                partial = scaled if partial is None else partial + scaled
            partial = partial.astype(jnp.bfloat16).astype(jnp.float32)
            total = partial if total is None else total + partial
        out_ref[tok] = total.astype(jnp.bfloat16)
        return carry

    lax.fori_loop(0, out_ref.shape[0], one_token, 0, unroll=4)


def combine(pos, gates, sources, per_group):
    tokens_dev, top_k = pos.shape
    count, subs, _ = sources[0].shape
    smem = pl.BlockSpec(memory_space=pltpu.SMEM)
    hbm = pl.BlockSpec(memory_space=pl.ANY)
    return pl.pallas_call(
        functools.partial(combine_kernel, per_group, top_k),
        in_specs=[smem, smem] + [hbm] * len(sources),
        out_specs=pl.BlockSpec(memory_space=pltpu.VMEM),
        out_shape=jax.ShapeDtypeStruct((tokens_dev, subs, LANES), jnp.bfloat16),
        scratch_shapes=[
            pltpu.VMEM((count * len(sources), subs, LANES), jnp.bfloat16),
            pltpu.SemaphoreType.DMA((len(sources),)),
        ],
        compiler_params=pltpu.CompilerParams(vmem_limit_bytes=60 * 2**20),
    )(pos.reshape(-1), gates.reshape(-1), *sources)


def solution(mesh):
    groups = mesh.shape['grp']
    inner_size = mesh.shape['ing']
    row_spec = P(('dp', 'grp', 'ing'), None)
    weight_spec = P(('grp', 'ing'), None, None)
    ahead = [(i, (i + 1) % inner_size) for i in range(inner_size)]
    behind = [(i, (i - 1) % inner_size) for i in range(inner_size)]

    def move(w, pairs):
        return lax.ppermute(w, 'ing', pairs)

    def device_step(tokens, expert_ids, gate_weights, w_gate, w_up, w_down):
        tokens_dev, dim = tokens.shape
        top_k = expert_ids.shape[1]
        local_exp = w_gate.shape[0]
        group_exp = local_exp * inner_size
        experts = group_exp * groups
        half = dim // 2
        per_group, expert_cap = cap_sizes(tokens_dev, top_k, groups, group_exp)
        inner = lax.axis_index('ing')

        own = [(w_gate[e], w_up[e], w_down[e][:, :half], w_down[e][:, half:]) for e in range(local_exp)]
        left = [tuple(move(w, ahead) for w in own[e]) for e in range(local_exp)]
        right = [tuple(move(w, behind) for w in own[e]) for e in range(local_exp)]
        far = [tuple(move((left, right)[k % 2][e][k], (ahead, behind)[k % 2]) for k in range(len(own[e]))) for e in range(local_exp)]

        shifts = (0, -1, 1, 2)
        held = {0: own, -1: left, 1: right, 2: far}
        phases = [(0, e) for e in range(local_exp)]
        phases += [(s, e) for e in range(local_exp) for s in (-1, 1)]
        phases += [(2, e) for e in range(local_exp)]
        assert inner_size == len(shifts)

        rows_all = lax.all_gather(tokens, 'grp', tiled=True)
        picked = jnp.any(expert_ids[:, :, None] == jnp.arange(experts), axis=1)
        before = jnp.tril(jnp.ones((tokens_dev, tokens_dev), jnp.bfloat16))
        upto = jnp.dot(before, picked.astype(jnp.bfloat16), preferred_element_type=jnp.float32).astype(jnp.int32)
        slot_tok = jnp.sum((upto.T[:, None, :] <= jnp.arange(expert_cap)[None, :, None]).astype(jnp.int32), axis=2)
        slot_tok = jnp.minimum(slot_tok, tokens_dev - 1).reshape(groups, group_exp * expert_cap)
        slot_in = lax.all_to_all(slot_tok, 'grp', 0, 0, tiled=True).reshape(groups, group_exp, expert_cap)
        slot_in = slot_in + (jnp.arange(groups, dtype=jnp.int32) * tokens_dev)[:, None, None]

        order = jnp.sum((expert_ids[:, None, :] < expert_ids[:, :, None]).astype(jnp.int32), axis=2)
        pick = order[:, :, None] == jnp.arange(top_k)
        ids = jnp.sum(jnp.where(pick, expert_ids[:, :, None], 0), axis=1)
        gates = jnp.sum(jnp.where(pick, gate_weights[:, :, None], 0.0), axis=1)
        rank = jnp.sum(jnp.where(ids[:, :, None] == jnp.arange(experts), upto[:, None, :], 0), axis=2) - 1
        member = ids % group_exp
        phase = jnp.zeros_like(ids)
        for p, (shift, e) in enumerate(phases):
            phase = jnp.where(member == (inner + shift) % inner_size * local_exp + e, p, phase)
        pos = (phase * groups + ids // group_exp) * expert_cap + rank

        returned = []
        for shift, e in phases:
            which = (inner + shift) % inner_size * local_exp + e
            index = lax.dynamic_index_in_dim(slot_in, which, 1, keepdims=False).reshape(-1)
            rows = rows_all.at[index].get(mode='promise_in_bounds')
            out = expert_ffn(rows, *held[shift][e], tile=256)
            out = out.reshape(groups, expert_cap, dim // LANES, LANES)
            back = lax.all_to_all(out, 'grp', 0, 0, tiled=True)
            returned.append(back.reshape(groups * expert_cap, dim // LANES, LANES))
        return combine(pos, gates, returned, per_group).reshape(tokens_dev, dim)


    return jax.shard_map(device_step, mesh=mesh, in_specs=(row_spec, row_spec, row_spec, weight_spec, weight_spec, weight_spec), out_specs=row_spec, check_vma=False)
```

```python
import functools

import jax
import jax.numpy as jnp
from jax import lax
from jax.experimental import pallas as pl
from jax.experimental.pallas import tpu as pltpu
from jax.sharding import PartitionSpec as P


LANES = 128


def cap_sizes(tokens_dev, top_k, groups, group_exp):
    group_limit = min(groups // 2, top_k // 2)
    per_group = top_k // group_limit
    group_cap = 3 * tokens_dev * group_limit // (2 * groups)
    expert_cap = (group_cap * per_group + group_exp - 1) // group_exp
    return per_group, expert_cap


def gated_rows(x_ref, gate_ref, up_ref):
    rows = x_ref[...]
    act_gate = jnp.dot(rows, gate_ref[...], preferred_element_type=jnp.float32)
    act_up = jnp.dot(rows, up_ref[...], preferred_element_type=jnp.float32)
    return (act_gate * jax.nn.sigmoid(act_gate) * act_up).astype(jnp.bfloat16)


def down_rows(hidden, down_refs, out_ref):
    at = 0
    for down_ref in down_refs:
        subs = down_ref.shape[1] // LANES
        out = jnp.dot(hidden, down_ref[...], preferred_element_type=jnp.float32)
        out_ref[:, at:at + subs, :] = out.astype(jnp.bfloat16).reshape(out.shape[0], subs, LANES)
        at += subs


def ffn_kernel(x_ref, gate_ref, up_ref, *refs):
    down_rows(gated_rows(x_ref, gate_ref, up_ref), refs[:-1], refs[-1])


def hidden_kernel(x_ref, gate_ref, up_ref, out_ref):
    out_ref[...] = gated_rows(x_ref, gate_ref, up_ref)


def down_kernel(x_ref, *refs):
    down_rows(x_ref[...], refs[:-1], refs[-1])


def per_tile(kernel, rows, weights, out_tail, tile):
    count, dim = rows.shape
    weight_bytes = sum(2 * w.size for w in weights)
    out_size = count
    for n in out_tail:
        out_size *= n
    return pl.pallas_call(
        kernel,
        grid=(count // tile,),
        in_specs=[pl.BlockSpec((tile, dim), lambda i: (i, 0))] + [pl.BlockSpec(w.shape, lambda i: (0, 0)) for w in weights],
        out_specs=pl.BlockSpec((tile,) + out_tail, lambda i: (i,) + (0,) * len(out_tail)),
        out_shape=jax.ShapeDtypeStruct((count,) + out_tail, jnp.bfloat16),
        compiler_params=pltpu.CompilerParams(vmem_limit_bytes=56 * 2**20),
        cost_estimate=pl.CostEstimate(flops=count * weight_bytes, bytes_accessed=2 * rows.size + weight_bytes + 2 * out_size, transcendentals=0),
    )(rows, *weights)


def expert_ffn(rows, gate_w, up_w, downs, tile):
    return per_tile(ffn_kernel, rows, (gate_w, up_w) + downs, (sum(d.shape[1] for d in downs) // LANES, LANES), tile)


def expert_hidden(rows, gate_w, up_w, tile):
    return per_tile(hidden_kernel, rows, (gate_w, up_w), (gate_w.shape[1],), tile)


def expert_down(hidden, downs, tile):
    return per_tile(down_kernel, hidden, downs, (sum(d.shape[1] for d in downs) // LANES, LANES), tile)


def combine_kernel(per_group, top_k, part, pos_ref, gate_ref, *refs):
    sources, (out_ref, held, sems) = refs[:-3], refs[-3:]
    count, subs = sources[-1].shape[:2]
    copies = []
    for k, src in enumerate(sources):
        src = src if src.shape[1] == subs else src.at[:, pl.ds(part * subs, subs), :]
        copies.append(pltpu.make_async_copy(src, held.at[pl.ds(k * count, count)], sems.at[k]))
    for copy in copies:
        copy.start()
    for copy in copies:
        copy.wait()

    def one_token(tok, carry):
        total = None
        for first in range(0, top_k, per_group):
            partial = None
            for j in range(first, first + per_group):
                scaled = held[pos_ref[tok * top_k + j]].astype(jnp.float32) * gate_ref[tok * top_k + j]
                partial = scaled if partial is None else partial + scaled
            partial = partial.astype(jnp.bfloat16).astype(jnp.float32)
            total = partial if total is None else total + partial
        out_ref[tok] = total.astype(jnp.bfloat16)
        return carry

    lax.fori_loop(0, out_ref.shape[0], one_token, 0, unroll=4)


def combine(pos, gates, sources, part, per_group):
    tokens_dev, top_k = pos.shape
    count, subs, _ = sources[-1].shape
    smem = pl.BlockSpec(memory_space=pltpu.SMEM)
    hbm = pl.BlockSpec(memory_space=pl.ANY)
    return pl.pallas_call(
        functools.partial(combine_kernel, per_group, top_k, part),
        in_specs=[smem, smem] + [hbm] * len(sources),
        out_specs=pl.BlockSpec(memory_space=pltpu.VMEM),
        out_shape=jax.ShapeDtypeStruct((tokens_dev, subs, LANES), jnp.bfloat16),
        scratch_shapes=[
            pltpu.VMEM((count * len(sources), subs, LANES), jnp.bfloat16),
            pltpu.SemaphoreType.DMA((len(sources),)),
        ],
        compiler_params=pltpu.CompilerParams(vmem_limit_bytes=60 * 2**20),
        cost_estimate=pl.CostEstimate(flops=0, bytes_accessed=2 * count * subs * LANES * len(sources), transcendentals=0),
    )(pos.reshape(-1), gates.reshape(-1), *sources)


def solution(mesh):
    groups = mesh.shape['grp']
    inner_size = mesh.shape['ing']
    row_spec = P(('dp', 'grp', 'ing'), None)
    weight_spec = P(('grp', 'ing'), None, None)
    ahead = [(i, (i + 1) % inner_size) for i in range(inner_size)]
    behind = [(i, (i - 1) % inner_size) for i in range(inner_size)]
    chip_ahead = [(g, (g + 2) % groups) for g in range(groups)]
    chip_behind = [(g, (g - 2) % groups) for g in range(groups)]
    partner = [(g, g ^ 1) for g in range(groups)]

    def device_step(tokens, expert_ids, gate_weights, w_gate, w_up, w_down):
        tokens_dev, dim = tokens.shape
        top_k = expert_ids.shape[1]
        local_exp = w_gate.shape[0]
        group_exp = local_exp * inner_size
        experts = group_exp * groups
        group_id = lax.axis_index('grp')
        per_group, expert_cap = cap_sizes(tokens_dev, top_k, groups, group_exp)
        inner = lax.axis_index('ing')

        first = w_gate[0]
        first, rest_gate, rest_up, rest_down = lax.optimization_barrier((first, w_gate, w_up, w_down))
        own = [(first if e == 0 else rest_gate[e], rest_up[e], rest_down[e]) for e in range(local_exp)]
        left = [tuple(lax.ppermute(w, 'ing', ahead) for w in own[e]) for e in range(local_exp)]
        right = [tuple(lax.ppermute(w, 'ing', behind) for w in own[e]) for e in range(local_exp)]
        far = []
        for e in range(local_exp):
            gate_w = lax.ppermute(left[e][0], 'ing', ahead)
            up_w = lax.ppermute(right[e][1], 'ing', behind)
            pieces = 2 if e < local_exp - 1 else 4
            width = dim // pieces
            downs = []
            for q in range(pieces):
                source, pairs = ((left, ahead), (right, behind))[q % 2]
                downs.append(lax.ppermute(source[e][2][:, q * width:(q + 1) * width], 'ing', pairs))
            far.append((gate_w, up_w, tuple(downs)))

        shifts = (0, -1, 1, 2)
        whole = lambda side: [(w[0], w[1], (w[2],)) for w in side]
        held = {0: whole(own), -1: whole(left), 1: whole(right), 2: far}
        phases = [(0, e) for e in range(local_exp)]
        phases += [(s, e) for e in range(local_exp) for s in (-1, 1)]
        phases += [(2, e) for e in range(local_exp)]
        assert inner_size == len(shifts)

        mid = tokens_dev // 2
        from_back = lax.ppermute(tokens, 'grp', chip_ahead)
        from_front = lax.ppermute(tokens, 'grp', chip_behind)
        across = [lax.ppermute(from_back[:mid], 'grp', chip_ahead), lax.ppermute(from_front[mid:], 'grp', chip_behind)]
        same_core = [tokens, from_back, from_front] + across
        rows_all = jnp.concatenate(same_core + [lax.ppermute(t, 'grp', partner) for t in same_core], axis=0)
        source_id = jnp.arange(groups, dtype=jnp.int32)
        chip_gap = (source_id // 2 - group_id // 2) % (groups // 2)
        block = jnp.where(chip_gap == 0, 0, jnp.where(chip_gap == groups // 2 - 1, 1, jnp.where(chip_gap == 1, 2, 3)))
        block = block + groups // 2 * (source_id % 2 != group_id % 2).astype(jnp.int32)
        assert groups // 2 == 4
        picked = jnp.any(expert_ids[:, :, None] == jnp.arange(experts), axis=1)
        before = jnp.tril(jnp.ones((tokens_dev, tokens_dev), jnp.bfloat16))
        upto = jnp.dot(before, picked.astype(jnp.bfloat16), preferred_element_type=jnp.float32).astype(jnp.int32)
        slot_tok = jnp.sum((upto.T[:, None, :] <= jnp.arange(expert_cap)[None, :, None]).astype(jnp.int32), axis=2)
        slot_tok = jnp.minimum(slot_tok, tokens_dev - 1).reshape(groups, group_exp * expert_cap)
        slot_in = lax.all_to_all(slot_tok, 'grp', 0, 0, tiled=True).reshape(groups, group_exp, expert_cap)
        slot_in = slot_in + (block * tokens_dev)[:, None, None]

        order = jnp.sum((expert_ids[:, None, :] < expert_ids[:, :, None]).astype(jnp.int32), axis=2)
        pick = order[:, :, None] == jnp.arange(top_k)
        ids = jnp.sum(jnp.where(pick, expert_ids[:, :, None], 0), axis=1)
        gates = jnp.sum(jnp.where(pick, gate_weights[:, :, None], 0.0), axis=1)
        rank = jnp.sum(jnp.where(ids[:, :, None] == jnp.arange(experts), upto[:, None, :], 0), axis=2) - 1
        member = ids % group_exp
        phase = jnp.zeros_like(ids)
        for p, (shift, e) in enumerate(phases):
            phase = jnp.where(member == (inner + shift) % inner_size * local_exp + e, p, phase)
        pos = (phase * groups + ids // group_exp) * expert_cap + rank

        returned = []
        for p, (shift, e) in enumerate(phases):
            which = (inner + shift) % inner_size * local_exp + e
            index = lax.dynamic_index_in_dim(slot_in, which, 1, keepdims=False).reshape(-1)
            rows = rows_all.at[index].get(mode='promise_in_bounds')
            gate_w, up_w, downs = held[shift][e]
            if p < len(phases) - 1:
                outs = [expert_ffn(rows, gate_w, up_w, downs, 256)]
            else:
                hidden = expert_hidden(rows, gate_w, up_w, 256)
                outs = []
                for part in range(2):
                    outs.append(expert_down(hidden, downs[2 * part:2 * part + 2], 256))
            backs = []
            for out in outs:
                subs = out.shape[1]
                back = lax.all_to_all(out.reshape(groups, expert_cap, subs, LANES), 'grp', 0, 0, tiled=True)
                backs.append(back.reshape(groups * expert_cap, subs, LANES))
            returned.append(backs)
        sources = [backs[0] for backs in returned[:-1]]
        sides = []
        for part, back in enumerate(returned[-1]):
            sides.append(combine(pos, gates, sources + [back], part, per_group))
        return jnp.concatenate([side.reshape(tokens_dev, dim // 2) for side in sides], axis=1)


    return jax.shard_map(device_step, mesh=mesh, in_specs=(row_spec, row_spec, row_spec, weight_spec, weight_spec, weight_spec), out_specs=row_spec, check_vma=False)
```

```python
import functools

import jax
import jax.numpy as jnp
from jax import lax
from jax.experimental import pallas as pl
from jax.experimental.pallas import tpu as pltpu
from jax.sharding import PartitionSpec as P


LANES = 128


def cap_sizes(tokens_dev, top_k, groups, group_exp):
    group_limit = min(groups // 2, top_k // 2)
    per_group = top_k // group_limit
    group_cap = 3 * tokens_dev * group_limit // (2 * groups)
    expert_cap = (group_cap * per_group + group_exp - 1) // group_exp
    return per_group, expert_cap


def gated_rows(x_ref, gate_ref, up_ref):
    rows = x_ref[...]
    act_gate = jnp.dot(rows, gate_ref[...], preferred_element_type=jnp.float32)
    act_up = jnp.dot(rows, up_ref[...], preferred_element_type=jnp.float32)
    return (act_gate * jax.nn.sigmoid(act_gate) * act_up).astype(jnp.bfloat16)


def down_rows(hidden, down_refs, out_ref):
    at = 0
    for down_ref in down_refs:
        subs = down_ref.shape[1] // LANES
        out = jnp.dot(hidden, down_ref[...], preferred_element_type=jnp.float32)
        out_ref[:, at:at + subs, :] = out.astype(jnp.bfloat16).reshape(out.shape[0], subs, LANES)
        at += subs


def ffn_kernel(x_ref, gate_ref, up_ref, *refs):
    down_rows(gated_rows(x_ref, gate_ref, up_ref), refs[:-1], refs[-1])


def hidden_kernel(x_ref, gate_ref, up_ref, out_ref):
    out_ref[...] = gated_rows(x_ref, gate_ref, up_ref)


def down_kernel(x_ref, *refs):
    down_rows(x_ref[...], refs[:-1], refs[-1])


def per_tile(kernel, rows, weights, out_tail, tile):
    weights = list(weights)
    count, dim = rows.shape
    specs = []
    weight_bytes = 0
    for k, w in enumerate(weights):
        w, e = w if isinstance(w, tuple) else (w, None)
        weights[k] = w
        weight_bytes += 2 * w.shape[-2] * w.shape[-1]
        specs.append(pl.BlockSpec(w.shape, lambda i: (0, 0)) if e is None else pl.BlockSpec((None,) + w.shape[1:], lambda i, e=e: (e, 0, 0)))
    out_size = count
    for n in out_tail:
        out_size *= n
    return pl.pallas_call(
        kernel,
        grid=(count // tile,),
        in_specs=[pl.BlockSpec((tile, dim), lambda i: (i, 0))] + specs,
        out_specs=pl.BlockSpec((tile,) + out_tail, lambda i: (i,) + (0,) * len(out_tail)),
        out_shape=jax.ShapeDtypeStruct((count,) + out_tail, jnp.bfloat16),
        compiler_params=pltpu.CompilerParams(vmem_limit_bytes=56 * 2**20),
        cost_estimate=pl.CostEstimate(flops=count * weight_bytes, bytes_accessed=2 * rows.size + weight_bytes + 2 * out_size, transcendentals=0),
    )(rows, *weights)


def expert_ffn(rows, gate_w, up_w, downs, tile):
    return per_tile(ffn_kernel, rows, (gate_w, up_w) + downs, (sum(d.shape[1] for d in downs) // LANES, LANES), tile)


def expert_hidden(rows, gate_w, up_w, tile):
    return per_tile(hidden_kernel, rows, (gate_w, up_w), (up_w.shape[1],), tile)


def expert_down(hidden, downs, tile):
    return per_tile(down_kernel, hidden, downs, (sum(d.shape[1] for d in downs) // LANES, LANES), tile)


def combine_kernel(per_group, top_k, part, pitch, pos_ref, gate_ref, *refs):
    ins, (out_ref, held, sums, sems) = refs[:-4], refs[-4:]
    sources = ins[:-1] if part else ins
    count, subs = sources[-1].shape[:2]
    tokens_dev = out_ref.shape[0]
    width = subs * LANES
    copies = []
    for k, src in enumerate(sources):
        src = src if src.shape[1] == subs else src.at[:, pl.ds(part * subs, subs), :]
        copies.append(pltpu.make_async_copy(src, held.at[pl.ds(k * count, count)], sems.at[k]))
    if part:
        copies.append(pltpu.make_async_copy(ins[-1], out_ref.at[:, pl.ds(0, width)], sems.at[len(sources)]))
    for copy in copies:
        copy.start()
    for copy in copies:
        copy.wait()

    def one_token(tok, carry):
        total = None
        for first in range(0, top_k, per_group):
            partial = None
            for j in range(first, first + per_group):
                gate = jnp.broadcast_to(gate_ref[tok, pl.ds(j, 1), :], (subs, LANES))
                scaled = held[pos_ref[tok * top_k + j]].astype(jnp.float32) * gate
                partial = scaled if partial is None else partial + scaled
            partial = partial.astype(jnp.bfloat16).astype(jnp.float32)
            total = partial if total is None else total + partial
        sums[pl.ds(tok, subs, stride=pitch), :] = total
        return carry

    lax.fori_loop(0, tokens_dev, one_token, 0, unroll=8)

    step = 128

    def one_block(block, carry):
        rows = pl.ds(pl.multiple_of(block * step, step), step)
        for c in range(subs):
            value = sums[pl.ds(pl.multiple_of(c * pitch + block * step, 8), step), :]
            out_ref[rows, pl.ds(part * width + c * LANES, LANES)] = value.astype(jnp.bfloat16)
        return carry

    lax.fori_loop(0, tokens_dev // step, one_block, 0)


def combine(pos, gates, sources, part, per_group, before):
    tokens_dev, top_k = pos.shape
    count, subs, _ = sources[-1].shape
    pitch = tokens_dev + 8
    ins = list(sources) + list(before)
    hbm = pl.BlockSpec(memory_space=pl.ANY)
    vmem = pl.BlockSpec(memory_space=pltpu.VMEM)
    return pl.pallas_call(
        functools.partial(combine_kernel, per_group, top_k, part, pitch),
        in_specs=[pl.BlockSpec(memory_space=pltpu.SMEM), vmem] + [hbm] * len(ins),
        out_specs=vmem,
        out_shape=jax.ShapeDtypeStruct((tokens_dev, (part + 1) * subs * LANES), jnp.bfloat16),
        scratch_shapes=[
            pltpu.VMEM((count * len(sources), subs, LANES), jnp.bfloat16),
            pltpu.VMEM((subs * pitch, LANES), jnp.float32),
            pltpu.SemaphoreType.DMA((len(ins),)),
        ],
        compiler_params=pltpu.CompilerParams(vmem_limit_bytes=127 * 2**19),
        cost_estimate=pl.CostEstimate(flops=0, bytes_accessed=2 * count * subs * LANES * len(sources), transcendentals=0),
    )(pos.reshape(-1), gates, *ins)


def solution(mesh):
    groups = mesh.shape['grp']
    inner_size = mesh.shape['ing']
    row_spec = P(('dp', 'grp', 'ing'), None)
    weight_spec = P(('grp', 'ing'), None, None)
    ahead = [(i, (i + 1) % inner_size) for i in range(inner_size)]
    behind = [(i, (i - 1) % inner_size) for i in range(inner_size)]
    chip_ahead = [(g, (g + 2) % groups) for g in range(groups)]
    chip_behind = [(g, (g - 2) % groups) for g in range(groups)]
    partner = [(g, g ^ 1) for g in range(groups)]

    def device_step(tokens, expert_ids, gate_weights, w_gate, w_up, w_down):
        tokens_dev, dim = tokens.shape
        top_k = expert_ids.shape[1]
        local_exp = w_gate.shape[0]
        group_exp = local_exp * inner_size
        experts = group_exp * groups
        group_id = lax.axis_index('grp')
        per_group, expert_cap = cap_sizes(tokens_dev, top_k, groups, group_exp)
        inner = lax.axis_index('ing')

        own = [(w_up[e], w_down[e]) for e in range(local_exp)]
        gate_left = lax.ppermute(w_gate, 'ing', ahead)
        gate_right = lax.ppermute(w_gate, 'ing', behind)
        left = [tuple(lax.ppermute(w, 'ing', ahead) for w in own[e]) for e in range(local_exp)]
        right = [tuple(lax.ppermute(w, 'ing', behind) for w in own[e]) for e in range(local_exp)]
        far = []
        for e in range(local_exp):
            gate_w = lax.ppermute(gate_left[e], 'ing', ahead)
            up_w = lax.ppermute(right[e][0], 'ing', behind)
            pieces = 2 if e < local_exp - 1 else 4
            width = dim // pieces
            downs = []
            for q in range(pieces):
                source, pairs = ((left, ahead), (right, behind))[q % 2]
                downs.append(lax.ppermute(source[e][1][:, q * width:(q + 1) * width], 'ing', pairs))
            far.append((gate_w, up_w, tuple(downs)))

        shifts = (0, -1, 1, 2)
        whole = lambda gate, side: [((gate, e), up, (down,)) for e, (up, down) in enumerate(side)]
        held = {0: whole(w_gate, own), -1: whole(gate_left, left), 1: whole(gate_right, right), 2: far}
        phases = [(0, e) for e in range(local_exp)]
        phases += [(s, e) for e in range(local_exp) for s in (-1, 1)]
        phases += [(2, e) for e in range(local_exp)]
        assert inner_size == len(shifts)

        mid = tokens_dev // 2
        from_back = lax.ppermute(tokens, 'grp', chip_ahead)
        from_front = lax.ppermute(tokens, 'grp', chip_behind)
        across = [lax.ppermute(from_back[:mid], 'grp', chip_ahead), lax.ppermute(from_front[mid:], 'grp', chip_behind)]
        same_core = [tokens, from_back, from_front] + across
        rows_all = jnp.concatenate(same_core + [lax.ppermute(t, 'grp', partner) for t in same_core], axis=0)
        source_id = jnp.arange(groups, dtype=jnp.int32)
        chip_gap = (source_id // 2 - group_id // 2) % (groups // 2)
        block = jnp.where(chip_gap == 0, 0, jnp.where(chip_gap == groups // 2 - 1, 1, jnp.where(chip_gap == 1, 2, 3)))
        block = block + groups // 2 * (source_id % 2 != group_id % 2).astype(jnp.int32)
        assert groups // 2 == 4
        picked = jnp.any(expert_ids[:, :, None] == jnp.arange(experts), axis=1)
        before = jnp.tril(jnp.ones((tokens_dev, tokens_dev), jnp.bfloat16))
        upto = jnp.dot(before, picked.astype(jnp.bfloat16), preferred_element_type=jnp.float32).astype(jnp.int32)
        slot_tok = jnp.sum((upto.T[:, None, :] <= jnp.arange(expert_cap)[None, :, None]).astype(jnp.int32), axis=2)
        slot_tok = jnp.minimum(slot_tok, tokens_dev - 1).reshape(groups, group_exp * expert_cap)
        slot_in = lax.all_to_all(slot_tok, 'grp', 0, 0, tiled=True).reshape(groups, group_exp, expert_cap)
        slot_in = slot_in + (block * tokens_dev)[:, None, None]

        order = jnp.sum((expert_ids[:, None, :] < expert_ids[:, :, None]).astype(jnp.int32), axis=2)
        pick = order[:, :, None] == jnp.arange(top_k)
        ids = jnp.sum(jnp.where(pick, expert_ids[:, :, None], 0), axis=1)
        gates = jnp.sum(jnp.where(pick, gate_weights[:, :, None], 0.0), axis=1)
        rank = jnp.sum(jnp.where(ids[:, :, None] == jnp.arange(experts), upto[:, None, :], 0), axis=2) - 1
        member = ids % group_exp
        phase = jnp.zeros_like(ids)
        for p, (shift, e) in enumerate(phases):
            phase = jnp.where(member == (inner + shift) % inner_size * local_exp + e, p, phase)
        pos = (phase * groups + ids // group_exp) * expert_cap + rank

        returned = []
        for p, (shift, e) in enumerate(phases):
            which = (inner + shift) % inner_size * local_exp + e
            index = lax.dynamic_index_in_dim(slot_in, which, 1, keepdims=False).reshape(-1)
            rows = rows_all.at[index].get(mode='promise_in_bounds')
            gate_w, up_w, downs = held[shift][e]
            if p < len(phases) - 1:
                outs = [expert_ffn(rows, gate_w, up_w, downs, 256)]
            else:
                hidden = expert_hidden(rows, gate_w, up_w, 256)
                outs = []
                for part in range(2):
                    outs.append(expert_down(hidden, downs[2 * part:2 * part + 2], 256))
            backs = []
            for out in outs:
                subs = out.shape[1]
                back = lax.all_to_all(out.reshape(groups, expert_cap, subs, LANES), 'grp', 0, 0, tiled=True)
                backs.append(back.reshape(groups * expert_cap, subs, LANES))
            returned.append(backs)
        sources = [backs[0] for backs in returned[:-1]]
        gates = jnp.broadcast_to(gates[:, :, None], gates.shape + (LANES,))
        out = []
        for part, back in enumerate(returned[-1]):
            out = [combine(pos, gates, sources + [back], part, per_group, out)]
        return out[0]

    return jax.shard_map(device_step, mesh=mesh, in_specs=(row_spec, row_spec, row_spec, weight_spec, weight_spec, weight_spec), out_specs=row_spec, check_vma=False)
```
